512 devices in a mesh: chan: 64 (over y_hi, z, core), tm: 8 (over x, y_lo).
Axes of the slice: x: 4, y: 8 (y_hi: 4, y_lo: 2; y = y_hi * 2 + y_lo), z: 8, core: 2. Of those that a mesh axis runs over, the one named last changes fastest.
Arguments:
- voltages: bfloat16 [2, 512, 256, 2048], P(None, None, 'chan', 'tm'), may hold values from -6 to 6, as said below
- flag_mask: int32 [16, 256], P('tm', 'chan'), may hold values from 0 to 1, as said below
- flagged_prefix_counts: int32 [16, 256], P('tm', 'chan'), may hold values from 0 to 127
Outputs:
- visibilities: float32 [512, 2, 256, 256], P(('chan', 'tm'))
The draws below stay inside these ranges and needn't reach their ends.
Inputs may be any that keep to these rules, and one draw needn't show every extreme that they name: `voltages`: samples that keep drops count as zero; a program may move only the kept samples, in any compact form. `flag_mask`: 1 keeps the block of 128 samples of an antenna, 0 drops it; some antennas are dropped in every block. The first flagged_prefix_counts samples of a kept block are flagged; flags and counts may be packed several to a word wherever they are moved.
All inputs are finite; a program needn't handle non-finite values.
Results may differ from the reference program's by a relative error of at most 0.0003.
Values may be sent and summed in bfloat16 or wider, within the bound.
No kernel may reach another device: no remote copies, remote signals or barrier semaphores. Data moves between devices by JAX's collectives and lax.ppermute only.
A program may use at most 64 MiB of HBM per device.

```python
import jax
import jax.numpy as jnp
from jax import lax

ANTENNA_COUNT = 256
CHANNEL_COUNT = 512
FLAG_BLOCK_WIDTH = 128
FLAG_BLOCK_COUNT = 16
SAMPLE_COUNT = 2048


def draw_voltages(key, part):
    value_key = jax.random.fold_in(key, 31)
    zero_key = jax.random.fold_in(key, 29)
    full_shape = (2, CHANNEL_COUNT, ANTENNA_COUNT, SAMPLE_COUNT)
    normal_values = jax.random.normal(value_key, full_shape, jnp.float32)
    values_drawn = jnp.clip(normal_values, -6.0, 6.0)
    silent = jax.random.randint(zero_key, (ANTENNA_COUNT, SAMPLE_COUNT), 0, 10) == 0
    return jnp.where(silent[None, None], 0.0, values_drawn).astype(jnp.bfloat16)


def draw_flag_mask(key, part):
    base = jax.random.fold_in(key, 17)
    initial_key, middle_key, final_key = jax.random.split(base, 3)
    valid_samples = (jax.random.randint(initial_key, (FLAG_BLOCK_COUNT, ANTENNA_COUNT), 0, 4) > 0).astype(jnp.int32)
    flagged_rows = jax.random.randint(middle_key, (ANTENNA_COUNT,), 0, 32) == 0
    selected_mask = jax.random.randint(final_key, (), 0, ANTENNA_COUNT)
    flagged_rows = flagged_rows | (jnp.arange(ANTENNA_COUNT) == selected_mask)
    return jnp.where(flagged_rows[None, :], 0, valid_samples).astype(jnp.int32)


def set_ends(result, rng, least, high):
    spot = [jax.random.randint(jax.random.fold_in(rng, axis), (), 0, length) for axis, length in enumerate(result.shape)]
    longest = result.shape.index(max(result.shape))
    neighbour = spot[:longest] + [(spot[longest] + 1) % result.shape[longest]] + spot[longest + 1:]
    return result.at[tuple(spot)].set(least).at[tuple(neighbour)].set(high)


def setup_inputs(seed: int = 0) -> dict:
    seeds = jax.random.split(jax.random.key(seed), 4)
    return {
        "voltages": draw_voltages(jax.random.fold_in(seeds[3], 71), 0),
        "flag_mask": draw_flag_mask(jax.random.fold_in(seeds[3], 71), 0),
        "flagged_prefix_counts": set_ends(jax.random.randint(seeds[2], (FLAG_BLOCK_COUNT, ANTENNA_COUNT), 0, FLAG_BLOCK_WIDTH), jax.random.fold_in(seeds[2], 1), 0, FLAG_BLOCK_WIDTH - 1).astype(jnp.int32),
    }


def pair_samples(flag_mask, flagged_prefix_counts):
    def add_block(total, block):
        live = block[0].astype(jnp.float32)
        cover = (FLAG_BLOCK_WIDTH - jnp.maximum(block[1][:, None], block[1][None, :])).astype(jnp.float32)
        return total + live[:, None] * live[None, :] * cover, 0

    start = jnp.zeros((flag_mask.shape[1], flag_mask.shape[1]), jnp.float32)
    total, unused = lax.scan(add_block, start, (flag_mask, flagged_prefix_counts))
    return total


def reference(voltages, flag_mask, flagged_prefix_counts):
    offsets = jnp.arange(FLAG_BLOCK_WIDTH, dtype=jnp.int32)
    retain_mask = (flag_mask.T[:, :, None] == 1) & (offsets[None, None, :] >= flagged_prefix_counts.T[:, :, None])
    retain_mask = retain_mask.reshape(ANTENNA_COUNT, SAMPLE_COUNT)
    width = 8

    def single_block(start):
        slab = lax.dynamic_slice_in_dim(voltages, start, width, 1)
        slab = jnp.where(retain_mask[None, None], slab, jnp.zeros((), slab.dtype)).astype(jnp.float32)
        real_part, imag_part = slab[0], slab[1]
        hp = lax.Precision.HIGHEST
        rr = jnp.einsum("cit,cjt->cij", real_part, real_part, precision=hp)
        ii = jnp.einsum("cit,cjt->cij", imag_part, imag_part, precision=hp)
        ir = jnp.einsum("cit,cjt->cij", imag_part, real_part, precision=hp)
        ri = jnp.einsum("cit,cjt->cij", real_part, imag_part, precision=hp)
        return jnp.stack([rr + ii, ir - ri], axis=1)

    block_offsets = jnp.arange(0, CHANNEL_COUNT, width, dtype=jnp.int32)
    visibility_matrix = lax.map(single_block, block_offsets).reshape(CHANNEL_COUNT, 2, ANTENNA_COUNT, ANTENNA_COUNT)
    pairs = pair_samples(flag_mask, flagged_prefix_counts)
    return visibility_matrix / jnp.maximum(pairs, 1.0)[None, None]
```

```python
import jax
import jax.numpy as jnp
from jax import lax
from jax.sharding import PartitionSpec as P

FLAG_BLOCK_WIDTH = 128
CODE_FLOOR = 8.0
CODE_BASE = 16.0


def first_kept(flag_mask, flagged_prefix_counts):
    return jnp.where(flag_mask == 1, flagged_prefix_counts, FLAG_BLOCK_WIDTH)


def shards(voltages, flag_mask, flagged_prefix_counts):
    parts, channels, ants, times = voltages.shape
    blocks = times // FLAG_BLOCK_WIDTH
    chan_devices = lax.axis_size("chan")
    time_devices = lax.axis_size("tm")
    first = first_kept(flag_mask, flagged_prefix_counts).T
    code = jnp.where(first > 0, first.astype(jnp.float32) + CODE_BASE, 0.0)
    code = code.astype(jnp.bfloat16)
    lane = jnp.arange(times, dtype=jnp.int32)
    code_line = jnp.repeat(code, FLAG_BLOCK_WIDTH, axis=1)
    put = (lane[None, :] % FLAG_BLOCK_WIDTH == 0) & (code_line > 0)
    real_part = jnp.where(put[None], code_line[None], voltages[0])
    line = jnp.stack([real_part, voltages[1]], axis=1)
    line = lax.all_to_all(line, ("chan", "tm"), 0, 0, tiled=True)
    line = line.reshape(chan_devices, time_devices, parts, ants, times)
    line = line.transpose(2, 0, 3, 1, 4).reshape(
        parts, chan_devices * ants, time_devices * blocks, FLAG_BLOCK_WIDTH
    )
    heads = line[0, :, :, 0].astype(jnp.float32)
    first = jnp.where(heads > CODE_FLOOR, heads - CODE_BASE, 0.0).astype(jnp.int32)
    offsets = jnp.arange(FLAG_BLOCK_WIDTH, dtype=jnp.int32)
    keep = (offsets >= first[:, :, None]).reshape(chan_devices * ants, -1)
    line = line.reshape(parts, chan_devices * ants, -1)
    line = jnp.where(keep[None], line, jnp.zeros((), line.dtype))
    keep = keep.astype(jnp.bfloat16)

    def gram(a, b):
        return jnp.einsum("it,jt->ij", a, b, preferred_element_type=jnp.float32)

    pairs = jnp.maximum(gram(keep, keep), 1.0)
    real_out = gram(line[0], line[0]) + gram(line[1], line[1])
    cross = gram(line[1], line[0])
    imag_out = cross - cross.T
    return (jnp.stack([real_out, imag_out]) / pairs[None])[None]


def solution(mesh):
    placed = (P(None, None, "chan", "tm"), P("tm", "chan"), P("tm", "chan"))
    return jax.shard_map(
        shards,
        mesh=mesh,
        in_specs=placed,
        out_specs=P(("chan", "tm"), None, None, None),
        check_vma=False,
    )
```

```python
import jax
import jax.numpy as jnp
from jax import lax
from jax.experimental import pallas as pl
from jax.experimental.pallas import tpu as pltpu
from jax.sharding import PartitionSpec as P

WIDTH = 128
CODE_FLOOR = 8.0
CODE_BASE = 16.0
PACK_STEPS = 8


def pack_kernel(mask_ref, count_ref, volt_ref, out_ref):
    parts, _, ants, times = volt_ref.shape
    blocks = times // WIDTH
    lane = lax.broadcasted_iota(jnp.int32, (ants, WIDTH), 1)
    row = lax.broadcasted_iota(jnp.int32, (ants, WIDTH), 0)
    for p in range(parts):
        for b in range(blocks):
            x = volt_ref[p, :, :, b * WIDTH : (b + 1) * WIDTH]
            if p == 0:
                code = jnp.zeros((ants, WIDTH), jnp.int32)
                for a in range(ants):
                    first = jnp.where(mask_ref[b, a] == 1, count_ref[b, a], WIDTH)
                    code = jnp.where(row == a, first, code)
                put = (lane == 0) & (code > 0)
                code = code.astype(jnp.float32) + CODE_BASE
                x = jnp.where(put[None], code[None], x.astype(jnp.float32)).astype(x.dtype)
            at = (p * blocks + b) * ants
            out_ref[:, at : at + ants, :] = x


def pack(voltages, flag_mask, counts):
    parts, channels, ants, times = voltages.shape
    step = channels // PACK_STEPS
    rows = parts * ants * times // WIDTH
    return pl.pallas_call(
        pack_kernel,
        grid=(PACK_STEPS,),
        in_specs=[
            pl.BlockSpec(memory_space=pltpu.SMEM),
            pl.BlockSpec(memory_space=pltpu.SMEM),
            pl.BlockSpec((parts, step, ants, times), lambda i: (0, i, 0, 0)),
        ],
        out_specs=pl.BlockSpec((step, rows, WIDTH), lambda i: (i, 0, 0)),
        out_shape=jax.ShapeDtypeStruct((channels, rows, WIDTH), voltages.dtype),
        name="pack",
    )(flag_mask, counts, voltages)


def gram_kernel(line_ref, out_ref, volt_scr, keep_scr, *, blocks):
    groups, rows, _ = line_ref.shape[0], line_ref.shape[2], WIDTH
    t = pl.program_id(0)
    ants = rows // (2 * blocks)
    all_ants = groups * ants
    lane = lax.broadcasted_iota(jnp.int32, (all_ants, WIDTH), 1).astype(jnp.float32)
    x = line_ref[:, 0].astype(jnp.float32)
    for b in range(blocks):
        re = x[:, b * ants : (b + 1) * ants].reshape(all_ants, WIDTH)
        at = (blocks + b) * ants
        im = x[:, at : at + ants].reshape(all_ants, WIDTH)
        head = re[:, 0:1]
        first = jnp.where(head > CODE_FLOOR, head - CODE_BASE, 0.0)
        keep = lane >= first
        slot = t * blocks + b
        volt_scr[0, slot] = jnp.where(keep, re, 0.0).astype(volt_scr.dtype)
        volt_scr[1, slot] = jnp.where(keep, im, 0.0).astype(volt_scr.dtype)
        keep_scr[slot] = jnp.where(keep, 1.0, 0.0).astype(keep_scr.dtype)

    @pl.when(t == pl.num_programs(0) - 1)
    def _():
        def dot(a, b):
            return lax.dot_general(a, b, (((1,), (1,)), ((), ())), preferred_element_type=jnp.float32)

        slots = volt_scr.shape[1]
        zero = jnp.zeros((all_ants, all_ants), jnp.float32)
        real_out, cross, pairs = zero, zero, zero
        for s in range(slots):
            re, im, keep = volt_scr[0, s], volt_scr[1, s], keep_scr[s]
            real_out = real_out + dot(re, re) + dot(im, im)
            cross = cross + dot(im, re)
            pairs = pairs + dot(keep, keep)
        pairs = jnp.maximum(pairs, 1.0)
        out_ref[0, 0] = real_out / pairs
        out_ref[0, 1] = (cross - cross.T) / pairs


def gram(line, time_devices, blocks, ants):
    groups = line.shape[0]
    rows = line.shape[2]
    all_ants = groups * ants
    slots = time_devices * blocks
    import functools

    return pl.pallas_call(
        functools.partial(gram_kernel, blocks=blocks),
        grid=(time_devices,),
        in_specs=[pl.BlockSpec((groups, 1, rows, WIDTH), lambda i: (0, i, 0, 0))],
        out_specs=pl.BlockSpec((1, 2, all_ants, all_ants), lambda i: (0, 0, 0, 0)),
        out_shape=jax.ShapeDtypeStruct((1, 2, all_ants, all_ants), jnp.float32),
        scratch_shapes=[
            pltpu.VMEM((2, slots, all_ants, WIDTH), jnp.bfloat16),
            pltpu.VMEM((slots, all_ants, WIDTH), jnp.bfloat16),
        ],
        name="gram",
    )(line)


def shards(voltages, flag_mask, flagged_prefix_counts):
    ants, times = voltages.shape[2:]
    chan_devices = lax.axis_size("chan")
    time_devices = lax.axis_size("tm")
    line = pack(voltages, flag_mask, flagged_prefix_counts)
    line = lax.all_to_all(line, ("chan", "tm"), 0, 0, tiled=True)
    line = line.reshape(chan_devices, time_devices, *line.shape[1:])
    return gram(line, time_devices, times // WIDTH, ants)


def solution(mesh):
    placed = (P(None, None, "chan", "tm"), P("tm", "chan"), P("tm", "chan"))
    return jax.shard_map(
        shards,
        mesh=mesh,
        in_specs=placed,
        out_specs=P(("chan", "tm"), None, None, None),
        check_vma=False,
    )
```

```python
import jax
import jax.numpy as jnp
from jax import lax
from jax.experimental import pallas as pl
from jax.experimental.pallas import tpu as pltpu
from jax.sharding import PartitionSpec as P

WIDTH = 128
CODE_FLOOR = 8.0
CODE_BASE = 16.0
PACK_CHUNKS = 4


def pack_kernel(mask_ref, count_ref, volt_ref, out_ref, scr, in_sem, out_sem):
    parts, channels, ants, times = volt_ref.shape
    blocks = times // WIDTH
    step = channels // PACK_CHUNKS

    def into(c, p):
        at = pl.ds(c * step, step)
        return pltpu.make_async_copy(volt_ref.at[p, at], scr.at[at, p], in_sem.at[c, p])

    def out(c):
        at = pl.ds(c * step, step)
        return pltpu.make_async_copy(scr.at[at], out_ref.at[at], out_sem.at[c])

    for c in range(PACK_CHUNKS):
        for p in range(parts):
            into(c, p).start()
    lane = lax.broadcasted_iota(jnp.int32, (ants, WIDTH), 1)
    row = lax.broadcasted_iota(jnp.int32, (ants, WIDTH), 0)
    puts, codes = [], []
    for b in range(blocks):
        code = jnp.zeros((ants, WIDTH), jnp.int32)
        for a in range(ants):
            first = jnp.where(mask_ref[b, a] == 1, count_ref[b, a], WIDTH)
            code = jnp.where(row == a, first, code)
        put = jnp.where((lane == 0) & (code > 0), 1.0, 0.0).astype(jnp.bfloat16)
        puts.append(put)
        codes.append((code.astype(jnp.float32) + CODE_BASE).astype(jnp.bfloat16))
    for c in range(PACK_CHUNKS):
        for p in range(parts):
            into(c, p).wait()
        for b in range(blocks):
            at = (pl.ds(c * step, step), 0, slice(None), pl.ds(b * WIDTH, WIDTH))
            scr[at] = jnp.where(puts[b][None] > 0.5, codes[b][None], scr[at])
        out(c).start()
    for c in range(PACK_CHUNKS):
        out(c).wait()


def pack(voltages, flag_mask, counts):
    parts, channels, ants, times = voltages.shape
    shape = (channels, parts, ants, times)
    return pl.pallas_call(
        pack_kernel,
        in_specs=[
            pl.BlockSpec(memory_space=pltpu.SMEM),
            pl.BlockSpec(memory_space=pltpu.SMEM),
            pl.BlockSpec(memory_space=pl.ANY),
        ],
        out_specs=pl.BlockSpec(memory_space=pl.ANY),
        out_shape=jax.ShapeDtypeStruct(shape, voltages.dtype),
        scratch_shapes=[
            pltpu.VMEM(shape, voltages.dtype),
            pltpu.SemaphoreType.DMA((PACK_CHUNKS, parts)),
            pltpu.SemaphoreType.DMA((PACK_CHUNKS,)),
        ],
        name="pack",
    )(flag_mask, counts, voltages)


def gram_kernel(line_ref, out_ref, line_scr, volt_scr, keep_scr, sem):
    groups, times_devices, parts, ants, times = line_ref.shape
    blocks = times // WIDTH
    all_ants = groups * ants
    samples = times_devices * times

    def into(t):
        return pltpu.make_async_copy(line_ref.at[:, t], line_scr.at[t], sem.at[t])

    for t in range(times_devices):
        into(t).start()
    lane = lax.broadcasted_iota(jnp.int32, (all_ants, WIDTH), 1).astype(jnp.float32)
    for t in range(times_devices):
        into(t).wait()
        for b in range(blocks):
            def piece(p):
                x = line_scr[t, :, p, :, b * WIDTH : (b + 1) * WIDTH]
                return x.astype(jnp.float32).reshape(all_ants, WIDTH)

            re, im = piece(0), piece(1)
            head = re[:, 0:1]
            keep = lane >= jnp.where(head > CODE_FLOOR, head - CODE_BASE, 0.0)
            at = t * times + b * WIDTH
            end = at + WIDTH
            volt_scr[:, at:end] = jnp.where(keep, re, 0.0).astype(volt_scr.dtype)
            volt_scr[:, samples + at : samples + end] = jnp.where(keep, im, 0.0).astype(volt_scr.dtype)
            keep_scr[:, at:end] = jnp.where(keep, 1.0, 0.0).astype(keep_scr.dtype)

    def dot(a, b):
        return lax.dot_general(a, b, (((1,), (1,)), ((), ())), preferred_element_type=jnp.float32)

    both, keep = volt_scr[...], keep_scr[...]
    scale = 1.0 / jnp.maximum(dot(keep, keep), 1.0)
    out_ref[0, 0] = dot(both, both) * scale
    cross = dot(both[:, samples:], both[:, :samples])
    out_ref[0, 1] = (cross - cross.T) * scale


def gram(line):
    groups, time_devices, parts, ants, times = line.shape
    all_ants = groups * ants
    samples = time_devices * times
    return pl.pallas_call(
        gram_kernel,
        in_specs=[pl.BlockSpec(memory_space=pl.ANY)],
        out_specs=pl.BlockSpec(memory_space=pltpu.VMEM),
        out_shape=jax.ShapeDtypeStruct((1, 2, all_ants, all_ants), jnp.float32),
        scratch_shapes=[
            pltpu.VMEM((time_devices, groups, parts, ants, times), line.dtype),
            pltpu.VMEM((all_ants, parts * samples), line.dtype),
            pltpu.VMEM((all_ants, samples), line.dtype),
            pltpu.SemaphoreType.DMA((time_devices,)),
        ],
        name="gram",
    )(line)


def shards(voltages, flag_mask, flagged_prefix_counts):
    chan_devices = lax.axis_size("chan")
    time_devices = lax.axis_size("tm")
    line = pack(voltages, flag_mask, flagged_prefix_counts)
    line = lax.all_to_all(line, ("chan", "tm"), 0, 0, tiled=True)
    return gram(line.reshape(chan_devices, time_devices, *line.shape[1:]))


def solution(mesh):
    placed = (P(None, None, "chan", "tm"), P("tm", "chan"), P("tm", "chan"))
    return jax.shard_map(
        shards,
        mesh=mesh,
        in_specs=placed,
        out_specs=P(("chan", "tm"), None, None, None),
        check_vma=False,
    )
```

```python
import jax
import jax.numpy as jnp
from jax import lax
from jax.experimental import pallas as pl
from jax.experimental.pallas import tpu as pltpu
from jax.sharding import PartitionSpec as P

WIDTH = 128
CODE_FLOOR = 8.0
CODE_BASE = 16.0
PACK_CHUNKS = 4
GRAM_TURNS = 2


def pack_kernel(mask_ref, count_ref, volt_ref, out_ref, scr, in_sem, out_sem):
    parts, channels, ants, times = volt_ref.shape
    blocks = times // WIDTH
    step = channels // PACK_CHUNKS

    def into(c, p):
        at = pl.ds(c * step, step)
        return pltpu.make_async_copy(volt_ref.at[p, at], scr.at[at, p], in_sem.at[c, p])

    def out(c):
        at = pl.ds(c * step, step)
        return pltpu.make_async_copy(scr.at[at], out_ref.at[at], out_sem.at[c])

    for c in range(PACK_CHUNKS):
        for p in range(parts):
            into(c, p).start()
    lane = lax.broadcasted_iota(jnp.int32, (ants, WIDTH), 1)
    row = lax.broadcasted_iota(jnp.int32, (ants, WIDTH), 0)
    puts, codes = [], []
    for b in range(blocks):
        code = jnp.zeros((ants, WIDTH), jnp.int32)
        for a in range(ants):
            first = jnp.where(mask_ref[b, a] == 1, count_ref[b, a], WIDTH)
            code = jnp.where(row == a, first, code)
        put = jnp.where((lane == 0) & (code > 0), 1.0, 0.0).astype(jnp.bfloat16)
        puts.append(put)
        codes.append((code.astype(jnp.float32) + CODE_BASE).astype(jnp.bfloat16))
    for c in range(PACK_CHUNKS):
        for p in range(parts):
            into(c, p).wait()
        for b in range(blocks):
            at = (pl.ds(c * step, step), 0, slice(None), pl.ds(b * WIDTH, WIDTH))
            scr[at] = jnp.where(puts[b][None] > 0.5, codes[b][None], scr[at])
        out(c).start()
    for c in range(PACK_CHUNKS):
        out(c).wait()


def pack(voltages, flag_mask, counts):
    parts, channels, ants, times = voltages.shape
    shape = (channels, parts, ants, times)
    return pl.pallas_call(
        pack_kernel,
        in_specs=[
            pl.BlockSpec(memory_space=pltpu.SMEM),
            pl.BlockSpec(memory_space=pltpu.SMEM),
            pl.BlockSpec(memory_space=pl.ANY),
        ],
        out_specs=pl.BlockSpec(memory_space=pl.ANY),
        out_shape=jax.ShapeDtypeStruct(shape, voltages.dtype),
        scratch_shapes=[
            pltpu.VMEM(shape, voltages.dtype),
            pltpu.SemaphoreType.DMA((PACK_CHUNKS, parts)),
            pltpu.SemaphoreType.DMA((PACK_CHUNKS,)),
        ],
        name="pack",
    )(flag_mask, counts, voltages)


def gram_kernel(line_ref, out_ref, volt_scr, keep_scr, out_scr, sem):
    groups, time_devices, _, ants, times = line_ref.shape
    blocks = times // WIDTH
    all_ants = groups * ants
    lane = lax.broadcasted_iota(jnp.int32, (all_ants, WIDTH), 1).astype(jnp.float32)

    def dot(a, b):
        return lax.dot_general(a, b, (((1,), (1,)), ((), ())), preferred_element_type=jnp.float32)

    def out(p):
        return pltpu.make_async_copy(out_scr.at[p], out_ref.at[0, p], sem.at[p])

    sums = None
    share = time_devices // GRAM_TURNS
    samples = share * times
    for turn in range(GRAM_TURNS):
        for t in range(share):
            for b in range(blocks):

                def piece(p):
                    x = line_ref[:, turn * share + t, p, :, b * WIDTH : (b + 1) * WIDTH]
                    return x.astype(jnp.float32).reshape(all_ants, WIDTH)

                re, im = piece(0), piece(1)
                head = re[:, 0:1]
                keep = lane >= jnp.where(head > CODE_FLOOR, head - CODE_BASE, 0.0)
                at = t * times + b * WIDTH
                end = at + WIDTH
                volt_scr[turn, :, at:end] = jnp.where(keep, re, 0.0).astype(volt_scr.dtype)
                volt_scr[turn, :, samples + at : samples + end] = jnp.where(keep, im, 0.0).astype(
                    volt_scr.dtype
                )
                keep_scr[turn, :, at:end] = jnp.where(keep, 1.0, 0.0).astype(keep_scr.dtype)
        both, keep = volt_scr[turn], keep_scr[turn]
        last = turn == GRAM_TURNS - 1
        parts = [lambda: dot(keep, keep), lambda: dot(both, both), lambda: dot(both[:, samples:], both[:, :samples])]
        if not last:
            fresh = [f() for f in parts]
            sums = fresh if sums is None else [x + y for x, y in zip(sums, fresh)]
        else:
            old = [0.0] * 3 if sums is None else sums
            scale = 1.0 / jnp.maximum(parts[0]() + old[0], 1.0)
            out_scr[0] = (parts[1]() + old[1]) * scale
            out(0).start()
            cross = parts[2]() + old[2]
            out_scr[1] = (cross - cross.T) * scale
            out(1).start()
    out(0).wait()
    out(1).wait()


def gram(line):
    groups, time_devices, parts, ants, times = line.shape
    all_ants = groups * ants
    samples = time_devices * times // GRAM_TURNS
    return pl.pallas_call(
        gram_kernel,
        in_specs=[pl.BlockSpec(memory_space=pltpu.VMEM)],
        out_specs=pl.BlockSpec(memory_space=pl.ANY),
        out_shape=jax.ShapeDtypeStruct((1, 2, all_ants, all_ants), jnp.float32),
        scratch_shapes=[
            pltpu.VMEM((GRAM_TURNS, all_ants, parts * samples), line.dtype),
            pltpu.VMEM((GRAM_TURNS, all_ants, samples), line.dtype),
            pltpu.VMEM((2, all_ants, all_ants), jnp.float32),
            pltpu.SemaphoreType.DMA((2,)),
        ],
        name="gram",
    )(line)


def pin(x):
    return pltpu.with_memory_space_constraint(x, pltpu.VMEM)


def shards(voltages, flag_mask, flagged_prefix_counts):
    chan_devices = lax.axis_size("chan")
    time_devices = lax.axis_size("tm")
    line = pack(voltages, flag_mask, flagged_prefix_counts)
    line = lax.all_to_all(line, ("chan", "tm"), 0, 0, tiled=True)
    line = line.reshape(chan_devices, time_devices, *line.shape[1:])
    return gram(pin(line))


def solution(mesh):
    placed = (P(None, None, "chan", "tm"), P("tm", "chan"), P("tm", "chan"))
    return jax.shard_map(
        shards,
        mesh=mesh,
        in_specs=placed,
        out_specs=P(("chan", "tm"), None, None, None),
        check_vma=False,
    )
```

```python
import functools

import jax
import jax.numpy as jnp
from jax import lax
from jax.experimental import pallas as pl
from jax.experimental.pallas import tpu as pltpu
from jax.sharding import PartitionSpec as P

WIDTH = 128
CODE_FLOOR = 8.0
CODE_BASE = 16.0
VMEM_LIMIT = 24 * 2**20
PACK_CHUNKS = 4
GRAM_TURNS = 2


def pack_kernel(mask_ref, count_ref, volt_ref, out_ref, in_sem):
    parts, channels, ants, times = volt_ref.shape
    blocks = times // WIDTH
    step = channels // PACK_CHUNKS

    def into(c, p):
        at = pl.ds(c * step, step)
        return pltpu.make_async_copy(volt_ref.at[p, at], out_ref.at[at, p], in_sem.at[c, p])

    for p in range(parts):
        for c in range(PACK_CHUNKS):
            into(c, p).start()
    lane = lax.broadcasted_iota(jnp.int32, (ants, WIDTH), 1)
    row = lax.broadcasted_iota(jnp.int32, (ants, WIDTH), 0)
    puts, codes = [], []
    for b in range(blocks):
        code = jnp.zeros((ants, WIDTH), jnp.int32)
        for a in range(ants):
            first = jnp.where(mask_ref[b, a] == 1, count_ref[b, a], WIDTH)
            code = jnp.where(row == a, first, code)
        put = jnp.where((lane == 0) & (code > 0), 1.0, 0.0).astype(jnp.bfloat16)
        puts.append(put)
        codes.append((code.astype(jnp.float32) + CODE_BASE).astype(jnp.bfloat16))
    for c in range(PACK_CHUNKS):
        into(c, 0).wait()
        for b in range(blocks):
            at = (pl.ds(c * step, step), 0, slice(None), pl.ds(b * WIDTH, WIDTH))
            out_ref[at] = jnp.where(puts[b][None] > 0.5, codes[b][None], out_ref[at])
    for c in range(PACK_CHUNKS):
        into(c, 1).wait()


def pack(voltages, flag_mask, counts):
    parts, channels, ants, times = voltages.shape
    shape = (channels, parts, ants, times)
    return pl.pallas_call(
        pack_kernel,
        in_specs=[
            pl.BlockSpec(memory_space=pltpu.SMEM),
            pl.BlockSpec(memory_space=pltpu.SMEM),
            pl.BlockSpec(memory_space=pltpu.HBM),
        ],
        out_specs=pl.BlockSpec(memory_space=pltpu.VMEM),
        out_shape=pltpu.VMEM(shape, voltages.dtype),
        scratch_shapes=[pltpu.SemaphoreType.DMA((PACK_CHUNKS, parts))],
        name="pack",
    )(flag_mask, counts, voltages)


def gram_kernel(flat_ref, out_ref, volt_scr, keep_scr, out_scr, sem, *, time_devices):
    parts, ants, times = flat_ref.shape[1:]
    line_ref = flat_ref.reshape(flat_ref.shape[0] // time_devices, time_devices, parts, ants, times)
    groups = line_ref.shape[0]
    blocks = times // WIDTH
    all_ants = groups * ants
    lane = lax.broadcasted_iota(jnp.int32, (all_ants, WIDTH), 1).astype(jnp.float32)

    def dot(a, b):
        return lax.dot_general(a, b, (((1,), (1,)), ((), ())), preferred_element_type=jnp.float32)

    def out(p):
        return pltpu.make_async_copy(out_scr.at[p], out_ref.at[0, p], sem.at[p])

    sums = None
    share = time_devices // GRAM_TURNS
    samples = share * times
    for turn in range(GRAM_TURNS):
        for t in range(share):
            for b in range(blocks):

                def piece(p):
                    x = line_ref[:, turn * share + t, p, :, b * WIDTH : (b + 1) * WIDTH]
                    return x.astype(jnp.float32).reshape(all_ants, WIDTH)

                re, im = piece(0), piece(1)
                head = re[:, 0:1]
                keep = lane >= jnp.where(head > CODE_FLOOR, head - CODE_BASE, 0.0)
                at = t * times + b * WIDTH
                end = at + WIDTH
                volt_scr[turn, :, at:end] = jnp.where(keep, re, 0.0).astype(volt_scr.dtype)
                volt_scr[turn, :, samples + at : samples + end] = jnp.where(keep, im, 0.0).astype(
                    volt_scr.dtype
                )
                keep_scr[turn, :, at:end] = jnp.where(keep, 1.0, 0.0).astype(keep_scr.dtype)
        both, keep = volt_scr[turn], keep_scr[turn]
        last = turn == GRAM_TURNS - 1
        sums_of = [lambda: dot(keep, keep), lambda: dot(both, both), lambda: dot(both[:, samples:], both[:, :samples])]
        if not last:
            fresh = [f() for f in sums_of]
            sums = fresh if sums is None else [x + y for x, y in zip(sums, fresh)]
        else:
            old = [0.0] * 3 if sums is None else sums
            scale = 1.0 / jnp.maximum(sums_of[0]() + old[0], 1.0)
            out_scr[0] = (sums_of[1]() + old[1]) * scale
            out(0).start()
            cross = sums_of[2]() + old[2]
            out_scr[1] = (cross - cross.T) * scale
            out(1).start()
    out(0).wait()
    out(1).wait()


def gram(line, time_devices):
    groups, parts, ants, times = line.shape
    groups = groups // time_devices
    all_ants = groups * ants
    samples = time_devices * times // GRAM_TURNS
    return pl.pallas_call(
        functools.partial(gram_kernel, time_devices=time_devices),
        in_specs=[pl.BlockSpec(memory_space=pltpu.VMEM)],
        out_specs=pl.BlockSpec(memory_space=pl.ANY),
        out_shape=jax.ShapeDtypeStruct((1, 2, all_ants, all_ants), jnp.float32),
        scratch_shapes=[
            pltpu.VMEM((GRAM_TURNS, all_ants, parts * samples), line.dtype),
            pltpu.VMEM((GRAM_TURNS, all_ants, samples), line.dtype),
            pltpu.VMEM((2, all_ants, all_ants), jnp.float32),
            pltpu.SemaphoreType.DMA((2,)),
        ],
        compiler_params=pltpu.CompilerParams(vmem_limit_bytes=VMEM_LIMIT),
        name="gram",
    )(line)


def pin(x):
    return pltpu.with_memory_space_constraint(x, pltpu.VMEM)


def shards(voltages, flag_mask, flagged_prefix_counts):
    time_devices = lax.axis_size("tm")
    line = pack(voltages, flag_mask, flagged_prefix_counts)
    line = lax.all_to_all(line, ("chan", "tm"), 0, 0, tiled=True)
    return gram(pin(line), time_devices)


def solution(mesh):
    placed = (P(None, None, "chan", "tm"), P("tm", "chan"), P("tm", "chan"))
    return jax.shard_map(
        shards,
        mesh=mesh,
        in_specs=placed,
        out_specs=P(("chan", "tm"), None, None, None),
        check_vma=False,
    )
```

```python
import functools

import jax
import jax.numpy as jnp
from jax import lax
from jax.experimental import pallas as pl
from jax.experimental.pallas import tpu as pltpu
from jax.sharding import PartitionSpec as P

WIDTH = 128
CODE_BASE = 16.0
VMEM_LIMIT = 24 * 2**20
PACK_CHUNKS = 4
GRAM_TURNS = 8


def pack_kernel(mask_ref, count_ref, volt_ref, out_ref, in_sem):
    parts, channels, ants, times = volt_ref.shape
    blocks = times // WIDTH
    step = channels // PACK_CHUNKS

    def into(c, p):
        at = pl.ds(c * step, step)
        return pltpu.make_async_copy(volt_ref.at[p, at], out_ref.at[at, p], in_sem.at[c, p])

    for p in range(parts):
        for c in range(PACK_CHUNKS):
            into(c, p).start()
    lane = lax.broadcasted_iota(jnp.int32, (ants, WIDTH), 1)
    row = lax.broadcasted_iota(jnp.int32, (ants, WIDTH), 0)
    puts, codes = [], []
    for b in range(blocks):
        code = jnp.zeros((ants, WIDTH), jnp.int32)
        for a in range(ants):
            first = jnp.where(mask_ref[b, a] == 1, count_ref[b, a], WIDTH)
            code = jnp.where(row == a, first, code)
        put = jnp.where((lane == 0) & (code > 0), 1.0, 0.0).astype(jnp.bfloat16)
        puts.append(put)
        codes.append((code.astype(jnp.float32) + CODE_BASE).astype(jnp.bfloat16))
    for c in range(PACK_CHUNKS):
        into(c, 0).wait()
        for b in range(blocks):
            at = (pl.ds(c * step, step), 0, slice(None), pl.ds(b * WIDTH, WIDTH))
            out_ref[at] = jnp.where(puts[b][None] > 0.5, codes[b][None], out_ref[at])
    for c in range(PACK_CHUNKS):
        into(c, 1).wait()


def pack(voltages, flag_mask, counts):
    parts, channels, ants, times = voltages.shape
    shape = (channels, parts, ants, times)
    return pl.pallas_call(
        pack_kernel,
        in_specs=[
            pl.BlockSpec(memory_space=pltpu.SMEM),
            pl.BlockSpec(memory_space=pltpu.SMEM),
            pl.BlockSpec(memory_space=pltpu.HBM),
        ],
        out_specs=pl.BlockSpec(memory_space=pltpu.VMEM),
        out_shape=pltpu.VMEM(shape, voltages.dtype),
        scratch_shapes=[pltpu.SemaphoreType.DMA((PACK_CHUNKS, parts))],
        name="pack",
    )(flag_mask, counts, voltages)


def gram_kernel(flat_ref, out_ref, volt_scr, keep_scr, out_scr, sem, *, time_devices):
    parts, ants, times = flat_ref.shape[1:]
    line_ref = flat_ref.reshape(flat_ref.shape[0] // time_devices, time_devices, parts, ants, times)
    groups = line_ref.shape[0]
    blocks = times // WIDTH
    all_ants = groups * ants
    lane_code = lax.broadcasted_iota(jnp.int32, (all_ants, WIDTH), 1).astype(jnp.float32) + CODE_BASE
    lane_code = lane_code.astype(jnp.bfloat16)
    zero = jnp.zeros((), jnp.bfloat16)
    one = jnp.ones((), jnp.bfloat16)

    def dot(a, b):
        return lax.dot_general(a, b, (((1,), (1,)), ((), ())), preferred_element_type=jnp.float32)

    def out(p):
        return pltpu.make_async_copy(out_scr.at[p], out_ref.at[0, p], sem.at[p])

    sums = None
    share = time_devices // GRAM_TURNS
    samples = share * times
    for turn in range(GRAM_TURNS):
        for t in range(share):
            for b in range(blocks):

                def piece(p):
                    x = line_ref[:, turn * share + t, p, :, b * WIDTH : (b + 1) * WIDTH]
                    return x.astype(jnp.float32).reshape(all_ants, WIDTH).astype(jnp.bfloat16)

                re, im = piece(0), piece(1)
                keep = lane_code >= re[:, 0:1]
                at = t * times + b * WIDTH
                end = at + WIDTH
                volt_scr[turn, :, at:end] = jnp.where(keep, re, zero)
                volt_scr[turn, :, samples + at : samples + end] = jnp.where(keep, im, zero)
                keep_scr[turn, :, at:end] = jnp.where(keep, one, zero)
        both, keep = volt_scr[turn], keep_scr[turn]
        last = turn == GRAM_TURNS - 1
        sums_of = [lambda: dot(keep, keep), lambda: dot(both, both), lambda: dot(both[:, samples:], both[:, :samples])]
        if not last:
            fresh = [f() for f in sums_of]
            sums = fresh if sums is None else [x + y for x, y in zip(sums, fresh)]
        else:
            old = [0.0] * 3 if sums is None else sums
            scale = 1.0 / jnp.maximum(sums_of[0]() + old[0], 1.0)
            out_scr[0] = (sums_of[1]() + old[1]) * scale
            out(0).start()
            cross = sums_of[2]() + old[2]
            out_scr[1] = (cross - cross.T) * scale
            out(1).start()
    out(0).wait()
    out(1).wait()


def gram(line, time_devices):
    groups, parts, ants, times = line.shape
    groups = groups // time_devices
    all_ants = groups * ants
    samples = time_devices * times // GRAM_TURNS
    return pl.pallas_call(
        functools.partial(gram_kernel, time_devices=time_devices),
        in_specs=[pl.BlockSpec(memory_space=pltpu.VMEM)],
        out_specs=pl.BlockSpec(memory_space=pl.ANY),
        out_shape=jax.ShapeDtypeStruct((1, 2, all_ants, all_ants), jnp.float32),
        scratch_shapes=[
            pltpu.VMEM((GRAM_TURNS, all_ants, parts * samples), line.dtype),
            pltpu.VMEM((GRAM_TURNS, all_ants, samples), line.dtype),
            pltpu.VMEM((2, all_ants, all_ants), jnp.float32),
            pltpu.SemaphoreType.DMA((2,)),
        ],
        compiler_params=pltpu.CompilerParams(vmem_limit_bytes=VMEM_LIMIT),
        name="gram",
    )(line)


def pin(x):
    return pltpu.with_memory_space_constraint(x, pltpu.VMEM)


def shards(voltages, flag_mask, flagged_prefix_counts):
    time_devices = lax.axis_size("tm")
    line = pack(voltages, flag_mask, flagged_prefix_counts)
    line = lax.all_to_all(line, ("chan", "tm"), 0, 0, tiled=True)
    return gram(pin(line), time_devices)


def solution(mesh):
    placed = (P(None, None, "chan", "tm"), P("tm", "chan"), P("tm", "chan"))
    return jax.shard_map(
        shards,
        mesh=mesh,
        in_specs=placed,
        out_specs=P(("chan", "tm"), None, None, None),
        check_vma=False,
    )
```

```python
import functools

import jax
import jax.numpy as jnp
from jax import lax
from jax.experimental import pallas as pl
from jax.experimental.pallas import tpu as pltpu
from jax.sharding import PartitionSpec as P

WIDTH = 128
CODE_BASE = 16.0
VMEM_LIMIT = 24 * 2**20
PACK_CHUNKS = 2
GRAM_TURNS = 8


def pack_kernel(mask_hbm, count_hbm, volt_ref, out_ref, mask_ref, count_ref, in_sem, flag_sem):
    parts, channels, rows, _ = volt_ref.shape
    blocks, ants = mask_ref.shape
    step = channels // PACK_CHUNKS

    def into(c, p):
        at = pl.ds(c * step, step)
        return pltpu.make_async_copy(volt_ref.at[p, at], out_ref.at[at, p], in_sem.at[c, p])

    flags = [
        pltpu.make_async_copy(mask_hbm, mask_ref, flag_sem.at[0]),
        pltpu.make_async_copy(count_hbm, count_ref, flag_sem.at[1]),
    ]
    for copy in flags:
        copy.start()
    for p in range(parts):
        for c in range(PACK_CHUNKS):
            into(c, p).start()
    for copy in flags:
        copy.wait()
    lane = lax.broadcasted_iota(jnp.int32, (rows, WIDTH), 1)
    row = lax.broadcasted_iota(jnp.int32, (rows, WIDTH), 0)
    code = jnp.zeros((rows, WIDTH), jnp.int32)
    for b in range(blocks):
        for a in range(ants):
            first = jnp.where(mask_ref[b, a] == 1, count_ref[b, a], WIDTH)
            code = jnp.where(row == b * ants + a, first, code)
    put = jnp.where((lane == 0) & (code > 0), 1.0, 0.0).astype(jnp.bfloat16)
    code = (code.astype(jnp.float32) + CODE_BASE).astype(jnp.bfloat16)
    for c in range(PACK_CHUNKS):
        into(c, 0).wait()
        at = (pl.ds(c * step, step), 0)
        out_ref[at] = jnp.where(put[None] > 0.5, code[None], out_ref[at])
    for c in range(PACK_CHUNKS):
        into(c, 1).wait()


def pack(voltages, flag_mask, counts):
    parts, channels, ants, times = voltages.shape
    blocks = times // WIDTH
    tiles = voltages.reshape(parts, channels, ants, blocks, WIDTH).transpose(0, 1, 3, 2, 4)
    tiles = tiles.reshape(parts, channels, blocks * ants, WIDTH)
    return pl.pallas_call(
        pack_kernel,
        in_specs=[
            pl.BlockSpec(memory_space=pltpu.HBM),
            pl.BlockSpec(memory_space=pltpu.HBM),
            pl.BlockSpec(memory_space=pltpu.HBM),
        ],
        out_specs=pl.BlockSpec(memory_space=pltpu.VMEM),
        out_shape=pltpu.VMEM((channels, parts, blocks * ants, WIDTH), voltages.dtype),
        scratch_shapes=[
            pltpu.SMEM(flag_mask.shape, flag_mask.dtype),
            pltpu.SMEM(counts.shape, counts.dtype),
            pltpu.SemaphoreType.DMA((PACK_CHUNKS, parts)),
            pltpu.SemaphoreType.DMA((2,)),
        ],
        name="pack",
    )(flag_mask, counts, tiles)


def gram_kernel(flat_ref, out_ref, volt_scr, keep_scr, out_scr, sem, *, time_devices, ants):
    parts, rows, _ = flat_ref.shape[1:]
    groups = flat_ref.shape[0] // time_devices
    line_ref = flat_ref.reshape(groups, time_devices, parts, rows, WIDTH)
    blocks = rows // ants
    all_ants = groups * ants
    lane_code = lax.broadcasted_iota(jnp.int32, (all_ants, WIDTH), 1).astype(jnp.float32) + CODE_BASE
    lane_code = lane_code.astype(jnp.bfloat16)
    upper = lax.broadcasted_iota(jnp.int32, (1, rows, WIDTH), 1) >= ants
    zero = jnp.zeros((), jnp.bfloat16)
    one = jnp.ones((), jnp.bfloat16)

    def dot(a, b):
        return lax.dot_general(a, b, (((1,), (1,)), ((), ())), preferred_element_type=jnp.float32)

    def out(p):
        return pltpu.make_async_copy(out_scr.at[p], out_ref.at[0, p], sem.at[p])

    def pieces(t, p):
        x = line_ref[:, t, p].astype(jnp.float32).reshape(groups // 2, 2, rows, WIDTH)
        even, odd = x[:, 0], x[:, 1]
        first = jnp.where(upper, pltpu.roll(odd, ants, 1), even)
        second = jnp.where(upper, odd, pltpu.roll(even, ants, 1))
        return [y.reshape(all_ants, WIDTH).astype(jnp.bfloat16) for y in (first, second)]

    sums = None
    share = time_devices // GRAM_TURNS
    samples = share * blocks * WIDTH
    for turn in range(GRAM_TURNS):
        for t in range(share):
            reals, imags = pieces(turn * share + t, 0), pieces(turn * share + t, 1)
            for b in range(blocks):
                re, im = reals[b], imags[b]
                keep = lane_code >= re[:, 0:1]
                at = (t * blocks + b) * WIDTH
                end = at + WIDTH
                volt_scr[turn, :, at:end] = jnp.where(keep, re, zero)
                volt_scr[turn, :, samples + at : samples + end] = jnp.where(keep, im, zero)
                keep_scr[turn, :, at:end] = jnp.where(keep, one, zero)
        both, keep = volt_scr[turn], keep_scr[turn]
        last = turn == GRAM_TURNS - 1
        sums_of = [lambda: dot(keep, keep), lambda: dot(both, both), lambda: dot(both[:, samples:], both[:, :samples])]
        if not last:
            fresh = [f() for f in sums_of]
            sums = fresh if sums is None else [x + y for x, y in zip(sums, fresh)]
        else:
            old = [0.0] * 3 if sums is None else sums
            scale = 1.0 / jnp.maximum(sums_of[0]() + old[0], 1.0)
            out_scr[0] = (sums_of[1]() + old[1]) * scale
            out(0).start()
            cross = sums_of[2]() + old[2]
            out_scr[1] = (cross - cross.T) * scale
            out(1).start()
    out(0).wait()
    out(1).wait()


def gram(line, time_devices, ants):
    senders, parts, rows, _ = line.shape
    groups = senders // time_devices
    all_ants = groups * ants
    samples = time_devices // GRAM_TURNS * rows // ants * WIDTH
    return pl.pallas_call(
        functools.partial(gram_kernel, time_devices=time_devices, ants=ants),
        in_specs=[pl.BlockSpec(memory_space=pltpu.VMEM)],
        out_specs=pl.BlockSpec(memory_space=pl.ANY),
        out_shape=jax.ShapeDtypeStruct((1, 2, all_ants, all_ants), jnp.float32),
        scratch_shapes=[
            pltpu.VMEM((GRAM_TURNS, all_ants, parts * samples), line.dtype),
            pltpu.VMEM((GRAM_TURNS, all_ants, samples), line.dtype),
            pltpu.VMEM((2, all_ants, all_ants), jnp.float32),
            pltpu.SemaphoreType.DMA((2,)),
        ],
        compiler_params=pltpu.CompilerParams(vmem_limit_bytes=VMEM_LIMIT),
        name="gram",
    )(line)


def pin(x):
    return pltpu.with_memory_space_constraint(x, pltpu.VMEM)


def shards(voltages, flag_mask, flagged_prefix_counts):
    time_devices = lax.axis_size("tm")
    line = pack(voltages, flag_mask, flagged_prefix_counts)
    line = lax.all_to_all(line, ("chan", "tm"), 0, 0, tiled=True)
    return gram(pin(line), time_devices, voltages.shape[2])


def solution(mesh):
    placed = (P(None, None, "chan", "tm"), P("tm", "chan"), P("tm", "chan"))
    return jax.shard_map(
        shards,
        mesh=mesh,
        in_specs=placed,
        out_specs=P(("chan", "tm"), None, None, None),
        check_vma=False,
    )
```

```python
import functools

import jax
import jax.numpy as jnp
from jax import lax
from jax.experimental import pallas as pl
from jax.experimental.pallas import tpu as pltpu
from jax.sharding import PartitionSpec as P

WIDTH = 128
CODE_BASE = 16.0
VMEM_LIMIT = 24 * 2**20
PACK_CHUNKS = 2
GRAM_TURNS = 8


def pack_kernel(mask_hbm, count_hbm, volt_ref, out_ref, mask_ref, count_ref, in_sem, flag_sem):
    parts, channels, rows, _ = volt_ref.shape
    blocks, ants = mask_ref.shape
    step = channels // PACK_CHUNKS

    def into(c, p):
        at = pl.ds(c * step, step)
        return pltpu.make_async_copy(volt_ref.at[p, at], out_ref.at[at, p], in_sem.at[c, p])

    flags = [
        pltpu.make_async_copy(mask_hbm, mask_ref, flag_sem.at[0]),
        pltpu.make_async_copy(count_hbm, count_ref, flag_sem.at[1]),
    ]
    for copy in flags:
        copy.start()
    for p in range(parts):
        for c in range(PACK_CHUNKS):
            into(c, p).start()
    for copy in flags:
        copy.wait()
    lane = lax.broadcasted_iota(jnp.int32, (rows, WIDTH), 1)
    row = lax.broadcasted_iota(jnp.int32, (rows, WIDTH), 0)
    code = jnp.zeros((rows, WIDTH), jnp.int32)
    for b in range(blocks):
        for a in range(ants):
            first = jnp.where(mask_ref[b, a] == 1, count_ref[b, a], WIDTH)
            code = jnp.where(row == b * ants + a, first, code)
    put = jnp.where((lane == 0) & (code > 0), 1.0, 0.0).astype(jnp.bfloat16)
    code = (code.astype(jnp.float32) + CODE_BASE).astype(jnp.bfloat16)
    for c in range(PACK_CHUNKS):
        into(c, 0).wait()
        at = (pl.ds(c * step, step), 0)
        out_ref[at] = jnp.where(put[None] > 0.5, code[None], out_ref[at])
    for c in range(PACK_CHUNKS):
        into(c, 1).wait()


def pack(voltages, flag_mask, counts):
    parts, channels, ants, times = voltages.shape
    blocks = times // WIDTH
    tiles = voltages.reshape(parts, channels, ants, blocks, WIDTH).transpose(0, 1, 3, 2, 4)
    tiles = tiles.reshape(parts, channels, blocks * ants, WIDTH)
    return pl.pallas_call(
        pack_kernel,
        in_specs=[
            pl.BlockSpec(memory_space=pltpu.HBM),
            pl.BlockSpec(memory_space=pltpu.HBM),
            pl.BlockSpec(memory_space=pltpu.HBM),
        ],
        out_specs=pl.BlockSpec(memory_space=pltpu.VMEM),
        out_shape=pltpu.VMEM((channels, parts, blocks * ants, WIDTH), voltages.dtype),
        scratch_shapes=[
            pltpu.SMEM(flag_mask.shape, flag_mask.dtype),
            pltpu.SMEM(counts.shape, counts.dtype),
            pltpu.SemaphoreType.DMA((PACK_CHUNKS, parts)),
            pltpu.SemaphoreType.DMA((2,)),
        ],
        name="pack",
    )(flag_mask, counts, tiles)


def gram_kernel(flat_ref, out_ref, volt_scr, keep_scr, out_scr, sem, *, time_devices, ants):
    parts, rows, _ = flat_ref.shape[1:]
    groups = flat_ref.shape[0] // time_devices
    line_ref = flat_ref.reshape(groups, time_devices, parts, rows, WIDTH)
    blocks = rows // ants
    all_ants = groups * ants
    lane_code = lax.broadcasted_iota(jnp.int32, (all_ants, WIDTH), 1).astype(jnp.float32) + CODE_BASE
    lane_code = lane_code.astype(jnp.bfloat16)
    zero = jnp.zeros((), jnp.bfloat16)
    one = jnp.ones((), jnp.bfloat16)

    def dot(a, b):
        return lax.dot_general(a, b, (((1,), (1,)), ((), ())), preferred_element_type=jnp.float32)

    def out(p):
        return pltpu.make_async_copy(out_scr.at[p], out_ref.at[0, p], sem.at[p])

    def pieces(t, p):
        x = line_ref[:, t, p].reshape(groups // 2, 2 * rows, WIDTH)

        def joined(b):
            near, far = b * ants, rows + b * ants
            pair = (x[:, near : near + ants], x[:, far : far + ants])
            return jnp.concatenate(pair, axis=1).reshape(all_ants, WIDTH)

        return [joined(b) for b in range(blocks)]

    sums = None
    share = time_devices // GRAM_TURNS
    samples = share * blocks * WIDTH
    for turn in range(GRAM_TURNS):
        for t in range(share):
            reals, imags = pieces(turn * share + t, 0), pieces(turn * share + t, 1)
            for b in range(blocks):
                re, im = reals[b], imags[b]
                keep = lane_code >= re[:, 0:1]
                at = (t * blocks + b) * WIDTH
                end = at + WIDTH
                volt_scr[turn, :, at:end] = jnp.where(keep, re, zero)
                volt_scr[turn, :, samples + at : samples + end] = jnp.where(keep, im, zero)
                keep_scr[turn, :, at:end] = jnp.where(keep, one, zero)
        both, keep = volt_scr[turn], keep_scr[turn]
        last = turn == GRAM_TURNS - 1
        sums_of = [lambda: dot(keep, keep), lambda: dot(both, both), lambda: dot(both[:, samples:], both[:, :samples])]
        if not last:
            fresh = [f() for f in sums_of]
            sums = fresh if sums is None else [x + y for x, y in zip(sums, fresh)]
        else:
            old = [0.0] * 3 if sums is None else sums
            scale = 1.0 / jnp.maximum(sums_of[0]() + old[0], 1.0)
            out_scr[0] = (sums_of[1]() + old[1]) * scale
            out(0).start()
            cross = sums_of[2]() + old[2]
            out_scr[1] = (cross - cross.T) * scale
            out(1).start()
    out(0).wait()
    out(1).wait()


def gram(line, time_devices, ants):
    senders, parts, rows, _ = line.shape
    groups = senders // time_devices
    all_ants = groups * ants
    samples = time_devices // GRAM_TURNS * rows // ants * WIDTH
    return pl.pallas_call(
        functools.partial(gram_kernel, time_devices=time_devices, ants=ants),
        in_specs=[pl.BlockSpec(memory_space=pltpu.VMEM)],
        out_specs=pl.BlockSpec(memory_space=pl.ANY),
        out_shape=jax.ShapeDtypeStruct((1, 2, all_ants, all_ants), jnp.float32),
        scratch_shapes=[
            pltpu.VMEM((GRAM_TURNS, all_ants, parts * samples), line.dtype),
            pltpu.VMEM((GRAM_TURNS, all_ants, samples), line.dtype),
            pltpu.VMEM((2, all_ants, all_ants), jnp.float32),
            pltpu.SemaphoreType.DMA((2,)),
        ],
        compiler_params=pltpu.CompilerParams(vmem_limit_bytes=VMEM_LIMIT),
        name="gram",
    )(line)


def pin(x):
    return pltpu.with_memory_space_constraint(x, pltpu.VMEM)


def shards(voltages, flag_mask, flagged_prefix_counts):
    time_devices = lax.axis_size("tm")
    line = pack(voltages, flag_mask, flagged_prefix_counts)
    line = lax.all_to_all(line, ("chan", "tm"), 0, 0, tiled=True)
    return gram(pin(line), time_devices, voltages.shape[2])


def solution(mesh):
    placed = (P(None, None, "chan", "tm"), P("tm", "chan"), P("tm", "chan"))
    return jax.shard_map(
        shards,
        mesh=mesh,
        in_specs=placed,
        out_specs=P(("chan", "tm"), None, None, None),
        check_vma=False,
    )
```
